32 devices in a mesh: seq: 8 (over y, x, core), stretch: 4 (over z).
Axes of the slice: x: 2, y: 2, z: 4, core: 2. Of those that a mesh axis runs over, the one named last changes fastest.
Arguments:
- queries: bfloat16 [4096, 1792], P(('stretch', 'seq')), may hold values from -140 to 140
- keys: bfloat16 [4096, 256], P(('stretch', 'seq')), may hold values from -6 to 6
- values: bfloat16 [4096, 256], P(('stretch', 'seq')), may hold values from -6 to 6
Outputs:
- attended: bfloat16 [4096, 1792], P(('stretch', 'seq'))
The draws below stay inside these ranges and needn't reach their ends.
All inputs are finite; a program needn't handle non-finite values.
Results may differ from the reference program's by a relative error of at most 0.011.
Values may be sent and summed in bfloat16 or wider, within the bound.
A program may use at most 64 MiB of HBM per device.

```python
import math
import jax
import jax.numpy as jnp
from jax import lax

QUERY_HEADS = 14
KEY_VALUE_HEADS = 2
HEAD_SIZE = 128
BLOCKS = 4
BLOCK_TOKENS = 1024
SEQS = 1
TOTAL_TOKENS = 4096


def base_keys(key):
    return jnp.clip(jax.random.normal(jax.random.fold_in(key, 11), (TOTAL_TOKENS, KEY_VALUE_HEADS * HEAD_SIZE), jnp.float32), -6.0, 6.0)


def draw_keys(key, part):
    rotary_base = base_keys(key)
    return rotary_base.astype(jnp.bfloat16)


def draw_queries(key, part):
    noise = 3.0 * jnp.clip(jax.random.normal(jax.random.fold_in(key, 17), (TOTAL_TOKENS, QUERY_HEADS * HEAD_SIZE), jnp.float32), -6.0, 6.0)
    return noise.astype(jnp.bfloat16)


def steps_of(key, dims, cuts, low, largest):
    gain = 1.0
    for position, parts in cuts:
        steps = jax.random.uniform(jax.random.fold_in(jax.random.fold_in(key, 6), position), (parts,), jnp.float32, low / len(cuts), largest / len(cuts))
        gain = gain * jnp.repeat(jnp.exp(steps), dims[position] // parts).reshape((-1,) + (1,) * (len(dims) - 1 - position))
    return gain


def bell_draw(stream_key, extent, width, most, cuts=(), kind=jnp.bfloat16):
    level = steps_of(stream_key, extent, cuts, -0.22, 0.18) if cuts else 1.0
    values = jax.random.normal(stream_key, extent, jnp.float32) * width * level
    return jnp.minimum(jnp.maximum(values, -most), most).astype(kind)


def setup_inputs(seed: int = 0) -> dict:
    key_of = jax.random.split(jax.random.key(seed), 4)
    return {
        "queries": draw_queries(jax.random.fold_in(key_of[3], 71), 0),
        "keys": draw_keys(jax.random.fold_in(key_of[3], 71), 0),
        "values": bell_draw(key_of[2], (TOTAL_TOKENS, KEY_VALUE_HEADS * HEAD_SIZE), 1.0, 6.0, ((0, 32),)),
    }


def apply_rotary(rows, token_positions, heads):
    half_width = HEAD_SIZE // 2
    inverse = 10000000.0 ** (-(jnp.arange(half_width, dtype=jnp.float32) * 2.0) / HEAD_SIZE)
    angles = token_positions.astype(jnp.float32)[:, None] * inverse[None, :]
    cosine = jnp.cos(angles)[:, None, :]
    sine_part = jnp.sin(angles)[:, None, :]
    shaped = rows.reshape(rows.shape[0], heads, HEAD_SIZE).astype(jnp.float32)
    first_half = shaped[..., :half_width]
    second_half = shaped[..., half_width:]
    turned = jnp.concatenate([first_half * cosine - second_half * sine_part, second_half * cosine + first_half * sine_part], axis=-1)
    return turned.reshape(rows.shape[0], heads * HEAD_SIZE).astype(jnp.bfloat16)

def reference(queries, keys, values):
    head_cluster = QUERY_HEADS // KEY_VALUE_HEADS
    score_scale = 1.0 / math.sqrt(HEAD_SIZE)
    rows_of_block = min(256, BLOCK_TOKENS)
    inner_position = jnp.arange(BLOCK_TOKENS, dtype=jnp.int32)
    outputs = [None] * (SEQS * BLOCKS)
    for sequence in range(SEQS):
        for block_position in range(BLOCKS):
            leading_row = (block_position * SEQS + sequence) * BLOCK_TOKENS
            query_rows = queries[leading_row:leading_row + BLOCK_TOKENS]
            rotated_sets = {'near': apply_rotary(query_rows, inner_position, QUERY_HEADS), 'next': apply_rotary(query_rows, inner_position + BLOCK_TOKENS, QUERY_HEADS), 'far': apply_rotary(query_rows, jnp.full((BLOCK_TOKENS,), 2 * BLOCK_TOKENS - 1, jnp.int32), QUERY_HEADS)}
            key_list = []
            value_list = []
            for source in range(block_position + 1):
                source_row = (source * SEQS + sequence) * BLOCK_TOKENS
                key_list.append(apply_rotary(keys[source_row:source_row + BLOCK_TOKENS], inner_position, KEY_VALUE_HEADS))
                value_list.append(values[source_row:source_row + BLOCK_TOKENS])
            rotated_keys = jnp.concatenate(key_list, axis=0).astype(jnp.float32).reshape(-1, KEY_VALUE_HEADS, HEAD_SIZE)
            rows_of_values = jnp.concatenate(value_list, axis=0).astype(jnp.float32).reshape(-1, KEY_VALUE_HEADS, HEAD_SIZE)

            def one_block(block_number, block_position=block_position, rotated_sets=rotated_sets, rotated_keys=rotated_keys, rows_of_values=rows_of_values):
                row_start = block_number * rows_of_block
                pieces = []
                for source in range(block_position + 1):
                    chosen = 'near' if source == block_position else 'next' if source == block_position - 1 else 'far'
                    block_of_query = lax.dynamic_slice_in_dim(rotated_sets[chosen], row_start, rows_of_block, 0)
                    block_of_query = block_of_query.astype(jnp.float32).reshape(rows_of_block, KEY_VALUE_HEADS, head_cluster, HEAD_SIZE)
                    key_block = rotated_keys[source * BLOCK_TOKENS:(source + 1) * BLOCK_TOKENS]
                    scores = jnp.einsum('rkgd,skd->kgrs', block_of_query, key_block, precision=lax.Precision.HIGHEST) * score_scale
                    if source == block_position:
                        allowed = (row_start + jnp.arange(rows_of_block, dtype=jnp.int32))[:, None] >= jnp.arange(BLOCK_TOKENS, dtype=jnp.int32)[None, :]
                        scores = jnp.where(allowed, scores, -1e+30)
                    pieces.append(scores)
                scores = jnp.concatenate(pieces, axis=-1)
                row_max = lax.optimization_barrier(jnp.max(scores, axis=-1, keepdims=True))
                weights = jnp.exp(scores - row_max)
                row_sum = lax.optimization_barrier(jnp.sum(weights, axis=-1))
                attended = jnp.einsum('kgrs,skd->rkgd', weights, rows_of_values, precision=lax.Precision.HIGHEST)
                attended = attended / jnp.transpose(row_sum, (2, 0, 1))[..., None]
                return attended.reshape(rows_of_block, QUERY_HEADS * HEAD_SIZE).astype(jnp.bfloat16)
            result = lax.map(one_block, jnp.arange(BLOCK_TOKENS // rows_of_block, dtype=jnp.int32))
            outputs[block_position * SEQS + sequence] = result.reshape(BLOCK_TOKENS, QUERY_HEADS * HEAD_SIZE)
    return jnp.concatenate(outputs, axis=0)
```

```python
import functools
import math

import jax
import jax.numpy as jnp
import numpy as np
from jax import lax
from jax.experimental import pallas as pl
from jax.experimental.pallas import tpu as pltpu
from jax.sharding import PartitionSpec as P

QUERY_HEADS = 14
KEY_VALUE_HEADS = 2
HEAD_SIZE = 128
BLOCKS = 4
CLUSTER = QUERY_HEADS // KEY_VALUE_HEADS
WIDTH = CLUSTER * HEAD_SIZE
SCALE = math.log2(math.e) / math.sqrt(HEAD_SIZE)


def rotary_table(positions):
    half = HEAD_SIZE // 2
    inverse = 10000000.0 ** (-(np.arange(half, dtype=np.float64) * 2.0) / HEAD_SIZE)
    angles = np.arange(positions, dtype=np.float64)[:, None] * inverse[None, :]
    return np.concatenate([np.cos(angles), np.sin(angles)], axis=1).astype(np.float32)


def factors(table):
    swapped = pltpu.roll(table, HEAD_SIZE // 2, 1)
    low = lax.broadcasted_iota(jnp.int32, table.shape, 1) < HEAD_SIZE // 2
    return jnp.where(low, table, swapped), jnp.where(low, -swapped, table)


def turned(rows, cosine, sine):
    x = rows.astype(jnp.float32)
    return (x * cosine + pltpu.roll(x, HEAD_SIZE // 2, 1) * sine).astype(jnp.bfloat16)


def kernel(
    shape, q_in, k_in, v_in, table_in, out,
    q_raw, q_rot, kv, k_rot, table, table_next, table_far, peak, total, acc, o_buf,
    local_sem, pair_send, pair_recv, slot_recv, chain_send, flat_send, relay_send,
    out_local, out_send, out_recv,
):
    shard, pairs, side_a, side_b, sequences, span = shape
    rows = 2 * shard
    length = pairs * rows
    s = lax.axis_index("seq")
    g = lax.axis_index("stretch")
    h = s % 2
    p = s // 2
    a = p // side_b
    b = p % side_b
    n = g // sequences
    partner = {"seq": s + 1 - 2 * h}
    above = {"stretch": g + sequences}
    below = {"stretch": g - sequences}
    mesh_type = pl.DeviceIdType.MESH

    def pair_at(a_index, b_index):
        return a_index * side_b + b_index

    def device_at(pair):
        return {"seq": 2 * pair + h}

    a_peers = [pair_at((a + j) % side_a, b) for j in range(1, side_a)]
    b_peers = [pair_at(a, (b + j) % side_b) for j in range(1, side_b)]
    diagonal = [
        pair_at((a + i) % side_a, (b + j) % side_b)
        for i in range(1, side_a)
        for j in range(1, side_b)
    ]

    def at(start, size, unit):
        return pl.ds(pl.multiple_of(start, unit), size)

    mine = at(h * shard, shard, shard)
    own_rows = at(p * rows + h * shard, shard, shard)

    def head_columns(head):
        return at(head * HEAD_SIZE, HEAD_SIZE, HEAD_SIZE)

    local = [
        (k_in.at[:, head_columns(h)], kv.at[0, 0, own_rows, :]),
        (v_in.at[:, head_columns(h)], kv.at[1, 0, own_rows, :]),
        (q_in.at[:, at(h * WIDTH, WIDTH, HEAD_SIZE)], q_raw.at[mine, :]),
        (table_in.at[pl.ds(0, length), :], table),
        (table_in.at[at(length + p * rows, rows, rows), :], table_next),
        (table_in.at[pl.ds(2 * length - 8, 8), :], table_far),
    ]
    local = [
        pltpu.make_async_copy(src, dst, local_sem.at[i]) for i, (src, dst) in enumerate(local)
    ]
    for copy in local:
        copy.start()

    barrier = pltpu.get_barrier_semaphore()

    def greet(device):
        pl.semaphore_signal(barrier, inc=1, device_id=device, device_id_type=mesh_type)

    greet(partner)
    for peer in a_peers + b_peers:
        greet(device_at(peer))

    @pl.when(n < BLOCKS - 1)
    def _():
        greet(above)

    @pl.when(n > 0)
    def _():
        greet(below)

    pl.semaphore_wait(
        barrier,
        1 + len(a_peers) + len(b_peers) + jnp.minimum(n, 1) + jnp.minimum(BLOCKS - 1 - n, 1),
    )

    swap = [
        (k_in.at[:, head_columns(1 - h)], kv.at[0, 0, own_rows, :]),
        (v_in.at[:, head_columns(1 - h)], kv.at[1, 0, own_rows, :]),
        (q_in.at[:, at((1 - h) * WIDTH, WIDTH, HEAD_SIZE)], q_raw.at[mine, :]),
    ]
    swap = [
        pltpu.make_async_remote_copy(
            src_ref=src, dst_ref=dst, send_sem=pair_send.at[i], recv_sem=pair_recv.at[i],
            device_id=partner, device_id_type=mesh_type,
        )
        for i, (src, dst) in enumerate(swap)
    ]
    for copy in swap:
        copy.start()

    def slot(t, d, pair):
        return kv.at[t, d, at(pair * rows, rows, rows), :]

    def message(t, d, pair, device, d_to, send_sem):
        return pltpu.make_async_remote_copy(
            src_ref=slot(t, d, pair), dst_ref=slot(t, d_to, pair),
            send_sem=send_sem, recv_sem=slot_recv.at[t, d_to, pair],
            device_id=device, device_id_type=mesh_type,
        )

    def arrived(t, d, pair):
        message(t, d, pair, partner, d, chain_send.at[0, 0]).wait_recv()

    def chain(t, d):
        return message(t, d, p, above, d + 1, chain_send.at[t, d])

    def flat(t, d):
        return [
            message(t, d, p, device_at(peer), d, flat_send.at[t, d, i])
            for i, peer in enumerate(b_peers + a_peers)
        ]

    def relays(t, d):
        sources, targets = (b_peers, a_peers) if t == 0 else (a_peers, b_peers)
        return [
            [
                message(t, d, source, device_at(target), d, relay_send.at[t, d, i, j])
                for j, target in enumerate(targets)
            ]
            for i, source in enumerate(sources)
        ]

    def column(d, first):
        for t in range(2):
            if first:
                local[t].wait()
                swap[t].wait_recv()
            else:
                arrived(t, d, p)

            @pl.when(n < BLOCKS - 1)
            def _():
                chain(t, d).start()

            for copy in flat(t, d):
                copy.start()

    def spread(d):
        for t, sources in ((0, b_peers), (1, a_peers)):
            for source, copies in zip(sources, relays(t, d)):
                arrived(t, d, source)
                for copy in copies:
                    copy.start()

    def settle(d):
        for t, sources in ((0, a_peers), (1, b_peers)):
            for source in sources + diagonal:
                arrived(t, d, source)

    def rotate_queries(cosine, sine):
        for c in range(CLUSTER):
            q_rot[c] = turned(q_raw[:, c * HEAD_SIZE : (c + 1) * HEAD_SIZE], cosine, sine)

    def rotate_keys(d):
        def tile(i, carry):
            where = at(i * rows, rows, rows)
            cosine, sine = factors(table[where, :])
            k_rot[where, :] = turned(kv[0, d, where, :], cosine, sine)
            return carry

        lax.fori_loop(0, pairs, tile, 0)

    def attend(d, causal):
        def step(group, carry):
            where = at(group * span, span, span)

            def head(c, inner):
                scores = lax.dot_general(
                    q_rot[c], k_rot[where, :], (((1,), (1,)), ((), ())),
                    preferred_element_type=jnp.float32,
                )
                if causal:
                    row = p * rows + lax.broadcasted_iota(jnp.int32, scores.shape, 0)
                    key = group * span + lax.broadcasted_iota(jnp.int32, scores.shape, 1)
                    scores = jnp.where(row >= key, scores, -1e30)
                old = peak[c]
                new = jnp.maximum(old, jnp.max(scores, axis=1, keepdims=True) * SCALE)
                peak[c] = new
                fade = jnp.exp2(old - new)
                top = new[:, :1]
                weights = jnp.exp2(scores * SCALE - top)
                part = weights[:, :HEAD_SIZE]
                for i in range(1, span // HEAD_SIZE):
                    part = part + weights[:, i * HEAD_SIZE : (i + 1) * HEAD_SIZE]
                total[c] = total[c] * fade + part
                acc[c] = acc[c] * fade + jnp.dot(
                    weights.astype(jnp.bfloat16), kv[1, d, where, :],
                    preferred_element_type=jnp.float32,
                )
                return inner

            lax.fori_loop(0, CLUSTER, head, 0)
            return carry

        lax.fori_loop(0, length // span, step, 0)

    column(0, True)
    peak[...] = jnp.full(peak.shape, -1e30, jnp.float32)
    total[...] = jnp.zeros(total.shape, jnp.float32)
    acc[...] = jnp.zeros(acc.shape, jnp.float32)
    for copy in local[2:]:
        copy.wait()
    swap[2].wait_recv()
    rotate_queries(*factors(table[at(p * rows, rows, rows), :]))
    spread(0)

    @pl.when(n > 0)
    def _():
        column(1, False)

    settle(0)
    rotate_keys(0)
    attend(0, True)

    def earlier(d, carry):
        @pl.when(d == 1)
        def _():
            rotate_queries(*factors(table_next[...]))

        @pl.when(d == 2)
        def _():
            cosine, sine = factors(table_far[...])
            rotate_queries(
                jnp.broadcast_to(cosine[7:8], (rows, HEAD_SIZE)),
                jnp.broadcast_to(sine[7:8], (rows, HEAD_SIZE)),
            )

        spread(d)

        @pl.when(d < n)
        def _():
            column(d + 1, False)

        settle(d)
        rotate_keys(d)
        attend(d, False)
        return carry

    lax.fori_loop(1, n + 1, earlier, 0)

    theirs = at((1 - h) * shard, shard, shard)

    def results(c):
        where = head_columns(h * CLUSTER + c)
        return (
            pltpu.make_async_copy(o_buf.at[c, mine, :], out.at[:, where], out_local.at[c]),
            pltpu.make_async_remote_copy(
                src_ref=o_buf.at[c, theirs, :], dst_ref=out.at[:, where],
                send_sem=out_send.at[c], recv_sem=out_recv.at[c],
                device_id=partner, device_id_type=mesh_type,
            ),
        )

    for c in range(CLUSTER + 1):
        if c < CLUSTER:
            under = jnp.sum(total[c], axis=1, keepdims=True)
            o_buf[c] = (acc[c] / under).astype(jnp.bfloat16)
        if c > 0:
            for copy in results(c - 1):
                copy.start()

    for copy in swap:
        copy.wait_send()

    def sent(d, carry):
        for t in range(2):
            @pl.when(n < BLOCKS - 1)
            def _():
                chain(t, d).wait_send()

            for copy in flat(t, d):
                copy.wait_send()
            for copies in relays(t, d):
                for copy in copies:
                    copy.wait_send()
        return carry

    lax.fori_loop(0, n + 1, sent, 0)
    for c in range(CLUSTER):
        here, there = results(c)
        here.wait()
        there.wait_send()
        there.wait_recv()


def on_device(queries, keys, values):
    shard = queries.shape[0]
    pairs = lax.axis_size("seq") // 2
    sequences = lax.axis_size("stretch") // BLOCKS
    side_a = max(i for i in range(1, pairs + 1) if pairs % i == 0 and i * i <= pairs)
    side_b = pairs // side_a
    rows = 2 * shard
    length = pairs * rows
    span = math.gcd(1024, length)
    shape = (shard, pairs, side_a, side_b, sequences, span)
    table = jnp.asarray(rotary_table(2 * length))
    dma = pltpu.SemaphoreType.DMA
    peers = max(side_a - 1 + side_b - 1, 1)
    most = max(side_b - 1, side_a - 1, 1)
    return pl.pallas_call(
        functools.partial(kernel, shape),
        out_shape=jax.ShapeDtypeStruct(queries.shape, jnp.bfloat16),
        in_specs=[pl.BlockSpec(memory_space=pl.ANY)] * 4,
        out_specs=pl.BlockSpec(memory_space=pl.ANY),
        scratch_shapes=[
            pltpu.VMEM((rows, WIDTH), jnp.bfloat16),
            pltpu.VMEM((CLUSTER, rows, HEAD_SIZE), jnp.bfloat16),
            pltpu.VMEM((2, BLOCKS, length, HEAD_SIZE), jnp.bfloat16),
            pltpu.VMEM((length, HEAD_SIZE), jnp.bfloat16),
            pltpu.VMEM((length, HEAD_SIZE), jnp.float32),
            pltpu.VMEM((rows, HEAD_SIZE), jnp.float32),
            pltpu.VMEM((8, HEAD_SIZE), jnp.float32),
            pltpu.VMEM((CLUSTER, rows, HEAD_SIZE), jnp.float32),
            pltpu.VMEM((CLUSTER, rows, HEAD_SIZE), jnp.float32),
            pltpu.VMEM((CLUSTER, rows, HEAD_SIZE), jnp.float32),
            pltpu.VMEM((CLUSTER, rows, HEAD_SIZE), jnp.bfloat16),
            dma((6,)),
            dma((3,)),
            dma((3,)),
            dma((2, BLOCKS, pairs)),
            dma((2, BLOCKS)),
            dma((2, BLOCKS, peers)),
            dma((2, BLOCKS, most, most)),
            dma((CLUSTER,)),
            dma((CLUSTER,)),
            dma((CLUSTER,)),
        ],
        compiler_params=pltpu.CompilerParams(
            collective_id=0, has_side_effects=True, vmem_limit_bytes=60 * 1024 * 1024
        ),
    )(queries, keys, values, table)


def solution(mesh):
    placed = P(("stretch", "seq"), None)
    return jax.shard_map(
        on_device, mesh=mesh, in_specs=(placed,) * 3, out_specs=placed, check_vma=False
    )
```

```python
import functools
import math

import jax
import jax.numpy as jnp
import numpy as np
from jax import lax
from jax.experimental import pallas as pl
from jax.experimental.pallas import tpu as pltpu
from jax.sharding import PartitionSpec as P

QUERY_HEADS = 14
KEY_VALUE_HEADS = 2
HEAD_SIZE = 128
BLOCKS = 4
CLUSTER = QUERY_HEADS // KEY_VALUE_HEADS
WIDTH = CLUSTER * HEAD_SIZE
UNROLL = CLUSTER
SCALE = math.log2(math.e) / math.sqrt(HEAD_SIZE)


def rotary_table(positions):
    half = HEAD_SIZE // 2
    inverse = 10000000.0 ** (-(np.arange(half, dtype=np.float64) * 2.0) / HEAD_SIZE)
    angles = np.arange(positions, dtype=np.float64)[:, None] * inverse[None, :]
    return np.concatenate([np.cos(angles), np.sin(angles)], axis=1).astype(np.float32)


def factors(table):
    swapped = pltpu.roll(table, HEAD_SIZE // 2, 1)
    low = lax.broadcasted_iota(jnp.int32, table.shape, 1) < HEAD_SIZE // 2
    return jnp.where(low, table, swapped), jnp.where(low, -swapped, table)


def turned(rows, cosine, sine):
    x = rows.astype(jnp.float32)
    return (x * cosine + pltpu.roll(x, HEAD_SIZE // 2, 1) * sine).astype(jnp.bfloat16)


def kernel(
    shape, q_in, k_in, v_in, table_in, out,
    q_raw, q_rot, kv, k_rot, table, table_next, table_far, peak, total, acc, o_buf,
    local_sem, pair_send, pair_recv, slot_recv, chain_send, flat_send, relay_send,
    out_local, out_send, out_recv,
):
    shard, pairs, side_a, side_b, sequences, span = shape
    rows = 2 * shard
    length = pairs * rows
    s = lax.axis_index("seq")
    g = lax.axis_index("stretch")
    h = s % 2
    p = s // 2
    a = p // side_b
    b = p % side_b
    n = g // sequences
    partner = {"seq": s + 1 - 2 * h}

    def block_at(shift):
        return {"stretch": g + shift * sequences}

    mesh_type = pl.DeviceIdType.MESH

    def pair_at(a_index, b_index):
        return a_index * side_b + b_index

    def device_at(pair):
        return {"seq": 2 * pair + h}

    a_peers = [pair_at((a + j) % side_a, b) for j in range(1, side_a)]
    b_peers = [pair_at(a, (b + j) % side_b) for j in range(1, side_b)]
    diagonal = [
        pair_at((a + i) % side_a, (b + j) % side_b)
        for i in range(1, side_a)
        for j in range(1, side_b)
    ]

    def at(start, size, unit):
        return pl.ds(pl.multiple_of(start, unit), size)

    mine = at(h * shard, shard, shard)
    own_rows = at(p * rows + h * shard, shard, shard)

    def head_columns(head):
        return at(head * HEAD_SIZE, HEAD_SIZE, HEAD_SIZE)

    local = [
        (k_in.at[:, head_columns(h)], kv.at[0, 0, own_rows, :]),
        (v_in.at[:, head_columns(h)], kv.at[1, 0, own_rows, :]),
        (q_in.at[:, at(h * WIDTH, WIDTH, HEAD_SIZE)], q_raw.at[mine, :]),
        (table_in.at[pl.ds(0, length), :], table),
        (table_in.at[at(length + p * rows, rows, rows), :], table_next),
        (table_in.at[pl.ds(2 * length - 8, 8), :], table_far),
    ]
    local = [
        pltpu.make_async_copy(src, dst, local_sem.at[i]) for i, (src, dst) in enumerate(local)
    ]
    for copy in local:
        copy.start()

    barrier = pltpu.get_barrier_semaphore()

    def greet(device):
        pl.semaphore_signal(barrier, inc=1, device_id=device, device_id_type=mesh_type)

    greet(partner)
    for peer in a_peers + b_peers:
        greet(device_at(peer))

    for k in range(1, BLOCKS):
        @pl.when(n + k < BLOCKS)
        def _():
            greet(block_at(k))

        @pl.when(n >= k)
        def _():
            greet(block_at(-k))

    pl.semaphore_wait(barrier, len(a_peers) + len(b_peers) + BLOCKS)

    swap = [
        (k_in.at[:, head_columns(1 - h)], kv.at[0, 0, own_rows, :]),
        (v_in.at[:, head_columns(1 - h)], kv.at[1, 0, own_rows, :]),
        (q_in.at[:, at((1 - h) * WIDTH, WIDTH, HEAD_SIZE)], q_raw.at[mine, :]),
    ]
    swap = [
        pltpu.make_async_remote_copy(
            src_ref=src, dst_ref=dst, send_sem=pair_send.at[i], recv_sem=pair_recv.at[i],
            device_id=partner, device_id_type=mesh_type,
        )
        for i, (src, dst) in enumerate(swap)
    ]
    for copy in swap:
        copy.start()

    def slot(t, d, pair):
        return kv.at[t, d, at(pair * rows, rows, rows), :]

    def message(t, d, pair, device, d_to, send_sem):
        return pltpu.make_async_remote_copy(
            src_ref=slot(t, d, pair), dst_ref=slot(t, d_to, pair),
            send_sem=send_sem, recv_sem=slot_recv.at[t, d_to, pair],
            device_id=device, device_id_type=mesh_type,
        )

    def arrived(t, d, pair):
        message(t, d, pair, partner, d, chain_send.at[0, 0]).wait_recv()

    def lift(t, k):
        return message(t, 0, p, block_at(k), k, chain_send.at[t, k])

    def flat(t, d):
        return [
            message(t, d, p, device_at(peer), d, flat_send.at[t, d, i])
            for i, peer in enumerate(b_peers + a_peers)
        ]

    def relays(t, d):
        sources, targets = (b_peers, a_peers) if t == 0 else (a_peers, b_peers)
        return [
            [
                message(t, d, source, device_at(target), d, relay_send.at[t, d, i, j])
                for j, target in enumerate(targets)
            ]
            for i, source in enumerate(sources)
        ]

    def column(d, first):
        for t in range(2):
            if first:
                local[t].wait()
                swap[t].wait_recv()
            else:
                arrived(t, d, p)

            if first:
                for k in range(BLOCKS - 1, 0, -1):
                    @pl.when(n + k < BLOCKS)
                    def _():
                        lift(t, k).start()

            for copy in flat(t, d):
                copy.start()

    def spread(d):
        for t, sources in ((0, b_peers), (1, a_peers)):
            for source, copies in zip(sources, relays(t, d)):
                arrived(t, d, source)
                for copy in copies:
                    copy.start()
        for t, sources in ((1, b_peers), (0, a_peers)):
            for source in sources:
                arrived(t, d, source)

    def settle(d):
        for t in range(2):
            for source in diagonal:
                arrived(t, d, source)

    def rotate_queries(version, cosine, sine):
        for c in range(CLUSTER):
            q_rot[version, c] = turned(
                q_raw[:, c * HEAD_SIZE : (c + 1) * HEAD_SIZE], cosine, sine
            )

    def attend(d, line, causal):
        where = at(line * span, span, span)
        version = jnp.minimum(d, 2)
        for i in range(side_b):
            tile = at(line * span + i * rows, rows, rows)
            cosine, sine = factors(table[tile, :])
            k_rot[i * rows : (i + 1) * rows, :] = turned(kv[0, d, tile, :], cosine, sine)

        def head(c, inner):
            scores = lax.dot_general(
                q_rot[version, c], k_rot[...], (((1,), (1,)), ((), ())),
                preferred_element_type=jnp.float32,
            )
            if causal:
                row = b * rows + lax.broadcasted_iota(jnp.int32, scores.shape, 0)
                key = lax.broadcasted_iota(jnp.int32, scores.shape, 1)
                scores = jnp.where(row >= key, scores, -1e30)
            new = jnp.max(scores, axis=1, keepdims=True) * SCALE
            if not causal:
                old = peak[c]
                new = jnp.maximum(old, new)
                fade = jnp.exp2(old - new)
                peak[c] = new
                new = new[:, :1]
            else:
                peak[c] = jnp.broadcast_to(new, (rows, HEAD_SIZE))
            weights = jnp.exp2(scores * SCALE - new)
            part = weights[:, :HEAD_SIZE]
            for i in range(1, span // HEAD_SIZE):
                part = part + weights[:, i * HEAD_SIZE : (i + 1) * HEAD_SIZE]
            product = jnp.dot(
                weights.astype(jnp.bfloat16), kv[1, d, where, :],
                preferred_element_type=jnp.float32,
            )
            total[c] = part if causal else total[c] * fade + part
            acc[c] = product if causal else acc[c] * fade + product
            return inner

        lax.fori_loop(0, CLUSTER, head, 0, unroll=UNROLL)

    column(0, True)
    for copy in local[2:]:
        copy.wait()
    swap[2].wait_recv()
    rotate_queries(0, *factors(table[at(p * rows, rows, rows), :]))
    spread(0)

    @pl.when(n > 0)
    def _():
        column(1, False)

    attend(0, a, True)
    rotate_queries(1, *factors(table_next[...]))
    cosine, sine = factors(table_far[...])
    rotate_queries(
        2,
        jnp.broadcast_to(cosine[7:8], (rows, HEAD_SIZE)),
        jnp.broadcast_to(sine[7:8], (rows, HEAD_SIZE)),
    )

    def block(d, carry):
        @pl.when(d + 1 <= n)
        def _():
            spread(d + 1)

        @pl.when(d + 2 <= n)
        def _():
            column(d + 2, False)

        settle(d)

        def visit(i, inner):
            line = (a + i) % side_a
            ahead = d + i // side_a

            @pl.when((ahead <= n) & ((d > 0) | (i == side_a) | (line < a)))
            def _():
                attend(ahead, line, False)

            return inner

        lax.fori_loop(1, side_a + 1, visit, 0)
        return carry

    lax.fori_loop(0, n + 1, block, 0)

    theirs = at((1 - h) * shard, shard, shard)

    def results(c):
        where = head_columns(h * CLUSTER + c)
        return (
            pltpu.make_async_copy(o_buf.at[c, mine, :], out.at[:, where], out_local.at[c]),
            pltpu.make_async_remote_copy(
                src_ref=o_buf.at[c, theirs, :], dst_ref=out.at[:, where],
                send_sem=out_send.at[c], recv_sem=out_recv.at[c],
                device_id=partner, device_id_type=mesh_type,
            ),
        )

    for c in range(CLUSTER + 1):
        if c < CLUSTER:
            under = jnp.sum(total[c], axis=1, keepdims=True)
            o_buf[c] = (acc[c] / under).astype(jnp.bfloat16)
        if c > 0:
            for copy in results(c - 1):
                copy.start()

    for copy in swap:
        copy.wait_send()

    def sent(d, carry):
        for t in range(2):
            for copy in flat(t, d):
                copy.wait_send()
            for copies in relays(t, d):
                for copy in copies:
                    copy.wait_send()
        return carry

    lax.fori_loop(0, n + 1, sent, 0)
    for t in range(2):
        for k in range(1, BLOCKS):
            @pl.when(n + k < BLOCKS)
            def _():
                lift(t, k).wait_send()

    for c in range(CLUSTER):
        here, there = results(c)
        here.wait()
        there.wait_send()
        there.wait_recv()


def on_device(queries, keys, values):
    shard = queries.shape[0]
    pairs = lax.axis_size("seq") // 2
    sequences = lax.axis_size("stretch") // BLOCKS
    side_a = max(i for i in range(1, pairs + 1) if pairs % i == 0 and i * i <= pairs)
    side_b = pairs // side_a
    rows = 2 * shard
    length = pairs * rows
    span = side_b * rows
    shape = (shard, pairs, side_a, side_b, sequences, span)
    table = jnp.asarray(rotary_table(2 * length))
    dma = pltpu.SemaphoreType.DMA
    peers = max(side_a - 1 + side_b - 1, 1)
    most = max(side_b - 1, side_a - 1, 1)
    return pl.pallas_call(
        functools.partial(kernel, shape),
        out_shape=jax.ShapeDtypeStruct(queries.shape, jnp.bfloat16),
        in_specs=[pl.BlockSpec(memory_space=pl.ANY)] * 4,
        out_specs=pl.BlockSpec(memory_space=pl.ANY),
        scratch_shapes=[
            pltpu.VMEM((rows, WIDTH), jnp.bfloat16),
            pltpu.VMEM((3, CLUSTER, rows, HEAD_SIZE), jnp.bfloat16),
            pltpu.VMEM((2, BLOCKS, length, HEAD_SIZE), jnp.bfloat16),
            pltpu.VMEM((span, HEAD_SIZE), jnp.bfloat16),
            pltpu.VMEM((length, HEAD_SIZE), jnp.float32),
            pltpu.VMEM((rows, HEAD_SIZE), jnp.float32),
            pltpu.VMEM((8, HEAD_SIZE), jnp.float32),
            pltpu.VMEM((CLUSTER, rows, HEAD_SIZE), jnp.float32),
            pltpu.VMEM((CLUSTER, rows, HEAD_SIZE), jnp.float32),
            pltpu.VMEM((CLUSTER, rows, HEAD_SIZE), jnp.float32),
            pltpu.VMEM((CLUSTER, rows, HEAD_SIZE), jnp.bfloat16),
            dma((6,)),
            dma((3,)),
            dma((3,)),
            dma((2, BLOCKS, pairs)),
            dma((2, BLOCKS)),
            dma((2, BLOCKS, peers)),
            dma((2, BLOCKS, most, most)),
            dma((CLUSTER,)),
            dma((CLUSTER,)),
            dma((CLUSTER,)),
        ],
        compiler_params=pltpu.CompilerParams(
            collective_id=0, has_side_effects=True, vmem_limit_bytes=60 * 1024 * 1024
        ),
    )(queries, keys, values, table)


def solution(mesh):
    placed = P(("stretch", "seq"), None)
    return jax.shard_map(
        on_device, mesh=mesh, in_specs=(placed,) * 3, out_specs=placed, check_vma=False
    )
```

```python
import functools
import math

import jax
import jax.numpy as jnp
import numpy as np
from jax import lax
from jax.experimental import pallas as pl
from jax.experimental.pallas import tpu as pltpu
from jax.sharding import PartitionSpec as P

QUERY_HEADS = 14
KEY_VALUE_HEADS = 2
HEAD_SIZE = 128
BLOCKS = 4
CLUSTER = QUERY_HEADS // KEY_VALUE_HEADS
WIDTH = CLUSTER * HEAD_SIZE
UNROLL = CLUSTER
SCALE = math.log2(math.e) / math.sqrt(HEAD_SIZE)


def rotary_table(positions):
    half = HEAD_SIZE // 2
    inverse = 10000000.0 ** (-(np.arange(half, dtype=np.float64) * 2.0) / HEAD_SIZE)
    angles = np.arange(positions, dtype=np.float64)[:, None] * inverse[None, :]
    return np.concatenate([np.cos(angles), np.sin(angles)], axis=1).astype(np.float32)


def factors(table):
    swapped = pltpu.roll(table, HEAD_SIZE // 2, 1)
    low = lax.broadcasted_iota(jnp.int32, table.shape, 1) < HEAD_SIZE // 2
    return jnp.where(low, table, swapped), jnp.where(low, -swapped, table)


def turned(rows, cosine, sine):
    x = rows.astype(jnp.float32)
    return (x * cosine + pltpu.roll(x, HEAD_SIZE // 2, 1) * sine).astype(jnp.bfloat16)


def kernel(
    shape, q_in, k_in, v_in, table_in, out,
    q_raw, q_rot, kv, k_rot, s_buf, w_buf, table, table_next, table_far, peak, total, acc, o_buf,
    local_sem, pair_send, pair_recv, slot_recv, chain_send, flat_send, relay_send,
    out_local, out_send, out_recv,
):
    shard, pairs, side_a, side_b, sequences, span = shape
    rows = 2 * shard
    length = pairs * rows
    s = lax.axis_index("seq")
    g = lax.axis_index("stretch")
    h = s % 2
    p = s // 2
    a = p // side_b
    b = p % side_b
    n = g // sequences
    partner = {"seq": s + 1 - 2 * h}

    def block_at(shift):
        return {"stretch": g + shift * sequences}

    mesh_type = pl.DeviceIdType.MESH

    def pair_at(a_index, b_index):
        return a_index * side_b + b_index

    def device_at(pair):
        return {"seq": 2 * pair + h}

    a_peers = [pair_at((a + j) % side_a, b) for j in range(1, side_a)]
    b_peers = [pair_at(a, (b + j) % side_b) for j in range(1, side_b)]
    diagonal = [
        pair_at((a + i) % side_a, (b + j) % side_b)
        for i in range(1, side_a)
        for j in range(1, side_b)
    ]

    def at(start, size, unit):
        return pl.ds(pl.multiple_of(start, unit), size)

    mine = at(h * shard, shard, shard)
    own_rows = at(p * rows + h * shard, shard, shard)

    def head_columns(head):
        return at(head * HEAD_SIZE, HEAD_SIZE, HEAD_SIZE)

    local = [
        (k_in.at[:, head_columns(h)], kv.at[0, 0, own_rows, :]),
        (v_in.at[:, head_columns(h)], kv.at[1, 0, own_rows, :]),
        (q_in.at[:, at(h * WIDTH, WIDTH, HEAD_SIZE)], q_raw.at[mine, :]),
        (table_in.at[pl.ds(0, length), :], table),
        (table_in.at[at(length + p * rows, rows, rows), :], table_next),
        (table_in.at[pl.ds(2 * length - 8, 8), :], table_far),
    ]
    local = [
        pltpu.make_async_copy(src, dst, local_sem.at[i]) for i, (src, dst) in enumerate(local)
    ]
    for copy in local:
        copy.start()

    barrier = pltpu.get_barrier_semaphore()

    def greet(device):
        pl.semaphore_signal(barrier, inc=1, device_id=device, device_id_type=mesh_type)

    greet(partner)
    for peer in a_peers + b_peers:
        greet(device_at(peer))

    for k in range(1, BLOCKS):
        @pl.when(n + k < BLOCKS)
        def _():
            greet(block_at(k))

        @pl.when(n >= k)
        def _():
            greet(block_at(-k))

    pl.semaphore_wait(barrier, len(a_peers) + len(b_peers) + BLOCKS)

    swap = [
        (k_in.at[:, head_columns(1 - h)], kv.at[0, 0, own_rows, :]),
        (v_in.at[:, head_columns(1 - h)], kv.at[1, 0, own_rows, :]),
        (q_in.at[:, at((1 - h) * WIDTH, WIDTH, HEAD_SIZE)], q_raw.at[mine, :]),
    ]
    swap = [
        pltpu.make_async_remote_copy(
            src_ref=src, dst_ref=dst, send_sem=pair_send.at[i], recv_sem=pair_recv.at[i],
            device_id=partner, device_id_type=mesh_type,
        )
        for i, (src, dst) in enumerate(swap)
    ]
    for copy in swap:
        copy.start()

    def slot(t, d, pair):
        return kv.at[t, d, at(pair * rows, rows, rows), :]

    def message(t, d, pair, device, d_to, send_sem):
        return pltpu.make_async_remote_copy(
            src_ref=slot(t, d, pair), dst_ref=slot(t, d_to, pair),
            send_sem=send_sem, recv_sem=slot_recv.at[t, d_to, pair],
            device_id=device, device_id_type=mesh_type,
        )

    def arrived(t, d, pair):
        message(t, d, pair, partner, d, chain_send.at[0, 0]).wait_recv()

    def lift(t, k):
        return message(t, 0, p, block_at(k), k, chain_send.at[t, k])

    def flat(t, d):
        return [
            message(t, d, p, device_at(peer), d, flat_send.at[t, d, i])
            for i, peer in enumerate(b_peers + a_peers)
        ]

    def relays(t, d):
        sources, targets = (b_peers, a_peers) if t == 0 else (a_peers, b_peers)
        return [
            [
                message(t, d, source, device_at(target), d, relay_send.at[t, d, i, j])
                for j, target in enumerate(targets)
            ]
            for i, source in enumerate(sources)
        ]

    def column(d, first):
        for t in range(2):
            if first:
                local[t].wait()
                swap[t].wait_recv()
            else:
                arrived(t, d, p)

            if first:
                for k in range(BLOCKS - 1, 0, -1):
                    @pl.when(n + k < BLOCKS)
                    def _():
                        lift(t, k).start()

            for copy in flat(t, d):
                copy.start()

    def spread(d):
        for t, sources in ((0, b_peers), (1, a_peers)):
            for source, copies in zip(sources, relays(t, d)):
                arrived(t, d, source)
                for copy in copies:
                    copy.start()
        for t, sources in ((1, b_peers), (0, a_peers)):
            for source in sources:
                arrived(t, d, source)

    def settle(d):
        for t in range(2):
            for source in diagonal:
                arrived(t, d, source)

    def rotate_queries(version, cosine, sine):
        for c in range(CLUSTER):
            q_rot[version, c] = turned(
                q_raw[:, c * HEAD_SIZE : (c + 1) * HEAD_SIZE], cosine, sine
            )

    def attend(d, line, causal):
        where = at(line * span, span, span)
        version = jnp.minimum(d, 2)
        for i in range(side_b):
            tile = at(line * span + i * rows, rows, rows)
            cosine, sine = factors(table[tile, :])
            k_rot[i * rows : (i + 1) * rows, :] = turned(kv[0, d, tile, :], cosine, sine)

        def score(c):
            s_buf[c % 2] = lax.dot_general(
                q_rot[version, c], k_rot[...], (((1,), (1,)), ((), ())),
                preferred_element_type=jnp.float32,
            )

        score(0)
        for c in range(CLUSTER):
            if c + 1 < CLUSTER:
                score(c + 1)
            for start in range(0, rows, 64):
                sub = slice(start, start + 64)
                scores = s_buf[c % 2, sub, :]
                if causal:
                    row = b * rows + start + lax.broadcasted_iota(jnp.int32, scores.shape, 0)
                    key = lax.broadcasted_iota(jnp.int32, scores.shape, 1)
                    scores = jnp.where(row >= key, scores, -1e30)
                new = jnp.max(scores, axis=1, keepdims=True) * SCALE
                if not causal:
                    old = peak[c, sub, :]
                    new = jnp.maximum(old, new)
                    fade = jnp.exp2(old - new)
                    peak[c, sub, :] = new
                    new = new[:, :1]
                else:
                    peak[c, sub, :] = jnp.broadcast_to(new, (64, HEAD_SIZE))
                weights = jnp.exp2(scores * SCALE - new)
                part = weights[:, :HEAD_SIZE]
                for i in range(1, span // HEAD_SIZE):
                    part = part + weights[:, i * HEAD_SIZE : (i + 1) * HEAD_SIZE]
                if causal:
                    total[c, sub, :] = part
                else:
                    total[c, sub, :] = total[c, sub, :] * fade + part
                    acc[c, sub, :] = acc[c, sub, :] * fade
                w_buf[c % 2, sub, :] = weights.astype(jnp.bfloat16)
            product = jnp.dot(
                w_buf[c % 2], kv[1, d, where, :], preferred_element_type=jnp.float32
            )
            acc[c] = product if causal else acc[c] + product

    column(0, True)
    for copy in local[2:]:
        copy.wait()
    swap[2].wait_recv()
    rotate_queries(0, *factors(table[at(p * rows, rows, rows), :]))
    spread(0)

    @pl.when(n > 0)
    def _():
        column(1, False)

    attend(0, a, True)
    rotate_queries(1, *factors(table_next[...]))
    cosine, sine = factors(table_far[...])
    rotate_queries(
        2,
        jnp.broadcast_to(cosine[7:8], (rows, HEAD_SIZE)),
        jnp.broadcast_to(sine[7:8], (rows, HEAD_SIZE)),
    )

    def block(d, carry):
        @pl.when(d + 1 <= n)
        def _():
            spread(d + 1)

        @pl.when(d + 2 <= n)
        def _():
            column(d + 2, False)

        settle(d)

        def visit(i, inner):
            line = (a + i) % side_a
            ahead = d + i // side_a

            @pl.when((ahead <= n) & ((d > 0) | (i == side_a) | (line < a)))
            def _():
                attend(ahead, line, False)

            return inner

        lax.fori_loop(1, side_a + 1, visit, 0)
        return carry

    lax.fori_loop(0, n + 1, block, 0)

    theirs = at((1 - h) * shard, shard, shard)

    def results(c):
        where = head_columns(h * CLUSTER + c)
        return (
            pltpu.make_async_copy(o_buf.at[c, mine, :], out.at[:, where], out_local.at[c]),
            pltpu.make_async_remote_copy(
                src_ref=o_buf.at[c, theirs, :], dst_ref=out.at[:, where],
                send_sem=out_send.at[c], recv_sem=out_recv.at[c],
                device_id=partner, device_id_type=mesh_type,
            ),
        )

    for c in range(CLUSTER + 1):
        if c < CLUSTER:
            under = jnp.sum(total[c], axis=1, keepdims=True)
            o_buf[c] = (acc[c] / under).astype(jnp.bfloat16)
        if c > 0:
            for copy in results(c - 1):
                copy.start()

    for copy in swap:
        copy.wait_send()

    def sent(d, carry):
        for t in range(2):
            for copy in flat(t, d):
                copy.wait_send()
            for copies in relays(t, d):
                for copy in copies:
                    copy.wait_send()
        return carry

    lax.fori_loop(0, n + 1, sent, 0)
    for t in range(2):
        for k in range(1, BLOCKS):
            @pl.when(n + k < BLOCKS)
            def _():
                lift(t, k).wait_send()

    for c in range(CLUSTER):
        here, there = results(c)
        here.wait()
        there.wait_send()
        there.wait_recv()


def on_device(queries, keys, values):
    shard = queries.shape[0]
    pairs = lax.axis_size("seq") // 2
    sequences = lax.axis_size("stretch") // BLOCKS
    side_a = max(i for i in range(1, pairs + 1) if pairs % i == 0 and i * i <= pairs)
    side_b = pairs // side_a
    rows = 2 * shard
    length = pairs * rows
    span = side_b * rows
    shape = (shard, pairs, side_a, side_b, sequences, span)
    table = jnp.asarray(rotary_table(2 * length))
    dma = pltpu.SemaphoreType.DMA
    peers = max(side_a - 1 + side_b - 1, 1)
    most = max(side_b - 1, side_a - 1, 1)
    return pl.pallas_call(
        functools.partial(kernel, shape),
        out_shape=jax.ShapeDtypeStruct(queries.shape, jnp.bfloat16),
        in_specs=[pl.BlockSpec(memory_space=pl.ANY)] * 4,
        out_specs=pl.BlockSpec(memory_space=pl.ANY),
        scratch_shapes=[
            pltpu.VMEM((rows, WIDTH), jnp.bfloat16),
            pltpu.VMEM((3, CLUSTER, rows, HEAD_SIZE), jnp.bfloat16),
            pltpu.VMEM((2, BLOCKS, length, HEAD_SIZE), jnp.bfloat16),
            pltpu.VMEM((span, HEAD_SIZE), jnp.bfloat16),
            pltpu.VMEM((2, rows, span), jnp.float32),
            pltpu.VMEM((2, rows, span), jnp.bfloat16),
            pltpu.VMEM((length, HEAD_SIZE), jnp.float32),
            pltpu.VMEM((rows, HEAD_SIZE), jnp.float32),
            pltpu.VMEM((8, HEAD_SIZE), jnp.float32),
            pltpu.VMEM((CLUSTER, rows, HEAD_SIZE), jnp.float32),
            pltpu.VMEM((CLUSTER, rows, HEAD_SIZE), jnp.float32),
            pltpu.VMEM((CLUSTER, rows, HEAD_SIZE), jnp.float32),
            pltpu.VMEM((CLUSTER, rows, HEAD_SIZE), jnp.bfloat16),
            dma((6,)),
            dma((3,)),
            dma((3,)),
            dma((2, BLOCKS, pairs)),
            dma((2, BLOCKS)),
            dma((2, BLOCKS, peers)),
            dma((2, BLOCKS, most, most)),
            dma((CLUSTER,)),
            dma((CLUSTER,)),
            dma((CLUSTER,)),
        ],
        compiler_params=pltpu.CompilerParams(
            collective_id=0, has_side_effects=True, vmem_limit_bytes=60 * 1024 * 1024
        ),
    )(queries, keys, values, table)


def solution(mesh):
    placed = P(("stretch", "seq"), None)
    return jax.shard_map(
        on_device, mesh=mesh, in_specs=(placed,) * 3, out_specs=placed, check_vma=False
    )
```
